512 devices in a mesh: expert: 32 (over z, y_hi), tensor: 16 (over y_lo, x, core).
Axes of the slice: x: 4, y: 8 (y_hi: 4, y_lo: 2; y = y_hi * 2 + y_lo), z: 8, core: 2. Of those that a mesh axis runs over, the one named last changes fastest.
Arguments:
- tokens: bfloat16 [4096, 3072], P('expert', 'tensor'), may hold values from -6 to 6
- expert_ids: int32 [4096, 2], P('expert'), may hold values from 0 to 7, all different within a row; in each aligned block of 128 rows (0 to 127, 128 to 255, ...) at most 48 rows name the same one
- joined_weight: bfloat16 [32, 3072, 2, 4096], P('expert', 'tensor'), may hold values from -0.109375 to 0.109375
Outputs:
- hidden: bfloat16 [4096, 2, 4, 4096], P('expert', None, None, 'tensor')
The draws below stay inside these ranges and needn't reach their ends.
Inputs may be any that keep to these rules, and one draw needn't show every extreme that they name: `expert_ids`: each row names 2 different experts. Among the rows of one device (each aligned block of 128 rows) no expert is named by more than 48 rows, and in some blocks one expert is named by exactly 48 rows.
All inputs are finite; a program needn't handle non-finite values.
Results may differ from the reference program's by a relative error of at most 0.001.
Values may be sent and summed in bfloat16 or wider, within the bound.
A program may use at most 128 MiB of HBM per device.

```python
import math
import jax
import jax.numpy as jnp
import numpy as np
from jax import lax

E = 8
TOP = 2
D = 3072
FF = 16384
TOK_DEV = 128
CAP = 48
REP = 4
FB = 4096
EB = 32
TOKENS = 4096


def levels(own_key, dims, cuts, low, high):
    loudness = 1.0
    for dim, blocks in cuts:
        steps = jax.random.uniform(jax.random.fold_in(jax.random.fold_in(own_key, 6), dim), (blocks,), jnp.float32, low / len(cuts), high / len(cuts))
        loudness = loudness * jnp.repeat(jnp.exp(steps), dims[dim] // blocks).reshape((-1,) + (1,) * (len(dims) - 1 - dim))
    return loudness


def shared_out(key, own, number, rows, amount, top, bound, lean):
    order = jax.random.permutation(key, amount)
    crowded, usual = load_shares(amount, rows * top, bound, lean, True), load_shares(amount, rows * top, bound, lean, False)
    places = jnp.arange(amount)

    def named(tallies, rotation):
        used = int((tallies > 0).sum())
        fixed = max(1, used // 4)
        passed = fixed + (places - fixed + rotation * (used - fixed)) % max(1, amount - fixed)
        return jnp.zeros((amount,), jnp.int32).at[order[jnp.where(places < fixed, places, passed)]].set(jnp.asarray(tallies, jnp.int32))

    tallies = jnp.where(number % 4 == 0, named(crowded, number // 4), named(usual, number - number // 4 - 1))
    mixed = jax.random.permutation(jax.random.fold_in(own, 3), amount)
    giver, sink = mixed[0:amount // 2 * 2:2], mixed[1:amount // 2 * 2:2]
    margin = jnp.minimum(tallies[giver] - 1, bound - tallies[sink]) // 2
    margin = jnp.where((giver == order[0]) | (sink == order[0]) | (tallies[sink] == 0), 0, jnp.maximum(margin, 0))
    passed = jax.random.randint(jax.random.fold_in(own, 4), (amount // 2,), 0, 1 << 20) % (margin + 1)
    tallies = tallies.at[giver].add(-passed).at[sink].add(passed)
    labels = jnp.searchsorted(jnp.cumsum(tallies), jnp.arange(rows * top), side="right").astype(jnp.int32)
    listing = labels.reshape(top, rows).T
    listing = listing[jax.random.permutation(jax.random.fold_in(own, 1), rows)]
    rotation = jax.random.randint(jax.random.fold_in(own, 2), (rows, 1), 0, top)
    return jnp.take_along_axis(listing, (jnp.arange(top)[None, :] + rotation) % top, axis=1)


def load_shares(amount, total, bound, lean, full):
    portions = [(1 << 20) // math.isqrt(standing ** lean) + 1 for standing in range(1, amount + 1)]
    largest = bound if full else min(bound, max(-(-total // amount), total * portions[0] // sum(portions)))
    least = 1 if total - largest >= amount - 1 else 0
    holding, spare = [largest] + [least] * (amount - 1), total - largest - least * (amount - 1)
    while spare > 0:
        free = [i for i in range(1, amount) if holding[i] < largest] or [i for i in range(1, amount) if holding[i] < bound]
        mass, remaining = sum([portions[i] for i in free]), spare
        for i in free:
            addition = min(bound - holding[i], max(1, remaining * portions[i] // mass), spare)
            holding[i] = holding[i] + addition
            spare = spare - addition
    return np.array(holding)


def gaussian(rng, shape, deviation, reach, split=(), kind=jnp.bfloat16):
    drawn = jax.random.normal(rng, shape, jnp.float32) * deviation
    if len(split) > 0:
        drawn = levels(rng, shape, split, -0.22, 0.18) * drawn
    return jnp.clip(drawn, min=-reach, max=reach).astype(kind)


def setup_inputs(seed: int = 0) -> dict:
    key_of = jax.random.split(jax.random.key(seed), 4)
    tokens = gaussian(key_of[0], (TOKENS, D), 1.0, 6.0, ((0, 32), (1, 16)))
    expert_ids_keys = jax.random.split(jax.random.fold_in(key_of[1], 1), TOKENS // TOK_DEV)
    expert_ids_turns = jax.random.permutation(jax.random.fold_in(key_of[1], 3), TOKENS // TOK_DEV)
    expert_ids = jax.vmap(lambda own, number: shared_out(jax.random.fold_in(key_of[1], 2), own, number, TOK_DEV, E, TOP, CAP, 2))(expert_ids_keys, expert_ids_turns).reshape((TOKENS, TOP))
    joined_weight = gaussian(key_of[2], (EB, D, 2, FB), D ** -0.5, 0.109375, ((0, 32), (1, 16)))
    return {"tokens": tokens, "expert_ids": expert_ids, "joined_weight": joined_weight}


def reference(tokens, expert_ids, joined_weight):
    sources = TOKENS // TOK_DEV
    flat_ids = expert_ids.reshape(sources, TOK_DEV * TOP)
    chosen = (flat_ids[:, :, None] == jnp.arange(E, dtype=jnp.int32)[None, None, :]).astype(jnp.int32)
    earlier = jnp.cumsum(chosen, axis=1) - chosen
    position = jnp.sum(earlier * chosen, axis=2).astype(jnp.int32)
    slot_index = (jnp.arange(sources, dtype=jnp.int32)[:, None] * CAP + position).reshape(-1).astype(jnp.int32)
    all_ids = flat_ids.reshape(-1)
    token_of = (jnp.arange(TOKENS * TOP, dtype=jnp.int32) // TOP).astype(jnp.int32)
    routed = tokens[token_of]

    def one_expert(index, result):
        expert = jnp.asarray(index).astype(jnp.int32)
        w_block = lax.dynamic_slice_in_dim(joined_weight, (expert * REP).astype(jnp.int32), REP, 0)
        weight = jnp.transpose(w_block, (1, 2, 0, 3)).reshape(D, 2 * FF)
        is_mine = all_ids == expert
        target = jnp.where(is_mine, slot_index, sources * CAP).astype(jnp.int32)
        buffer = jnp.zeros((sources * CAP + 1, D), jnp.bfloat16).at[target].set(routed)
        gate_up = jnp.dot(buffer, weight, preferred_element_type=jnp.float32)
        active = (jax.nn.silu(gate_up[:, :FF]) * gate_up[:, FF:]).astype(jnp.bfloat16)
        return jnp.where(is_mine[:, None], active[target], result)

    start_out = jnp.zeros((TOKENS * TOP, FF), jnp.bfloat16)
    result = lax.fori_loop(0, E, one_expert, start_out)
    return result.reshape(TOKENS, TOP, REP, FB)
```

```python
import functools

import jax
import jax.numpy as jnp
from jax import lax
from jax.experimental import pallas as pl
from jax.experimental.pallas import tpu as pltpu
from jax.sharding import PartitionSpec as P

MESH = pl.DeviceIdType.MESH
E = 8
CAP = 48
BF = jnp.bfloat16
F32 = jnp.float32


def kernel(
    tok_ref, ids_ref, idst_ref, w_ref, out_ref,
    xbuf, wrecv, wrelay, wk, tok_own, tok_oth, placed, slots, act, ret,
    ws, wr, rs, rr, fs, own_sem, ts, tr, zs, zr, zl,
    ys, yr, xs, xr, ds, dr, hs, hr, hl,
):
    a, b = lax.axis_index("expert"), lax.axis_index("tensor")
    z, yh = a // 4, a % 4
    yl, x, c = b // 8, (b // 2) % 4, b % 2
    y = 2 * yh + yl

    def dev(zz, yy, xx, cc):
        yy, xx, zz = yy % 8, xx % 4, zz % 8
        return (zz * 4 + yy // 2, (yy % 2) * 8 + xx * 2 + cc)

    yp = y + 1 - 2 * yl
    rows = w_ref.shape[0]
    half = 256

    def remote(src, dst, send, recv, to):
        return pltpu.make_async_remote_copy(
            src_ref=src, dst_ref=dst, send_sem=send, recv_sem=recv,
            device_id=to, device_id_type=MESH,
        )

    me = dev(z, y, x, 1 - c)

    def got(ref, sem):
        remote(ref, ref, sem, sem, me).wait_recv()

    def sent(ref, sem):
        remote(ref, ref, sem, sem, me).wait_send()

    barrier = pltpu.get_barrier_semaphore()
    count = 0

    def greet(to):
        pl.semaphore_signal(barrier, inc=1, device_id=to, device_id_type=MESH)

    for dx in range(4):
        for dy in range(2):
            for dc in range(2):
                if dx or dy or dc:
                    greet(dev(z, y if dy == 0 else yp, x + dx, c if dc == 0 else 1 - c))
                    count += 1
    for k in range(1, 8):
        greet(dev(z + k, y, x, c))
        count += 1
    greet(dev(z, y - 1 + 2 * yl, x, c))
    count += 1

    tok_own[...] = tok_ref[...]
    it = lax.broadcasted_iota
    ids_t = idst_ref[...]
    named = (ids_t[0:1, :] == it(jnp.int32, (8, 128), 0)) | (ids_t[1:2, :] == it(jnp.int32, (8, 128), 0))
    before = (it(jnp.int32, (128, 128), 0) < it(jnp.int32, (128, 128), 1)).astype(F32).astype(BF)
    earlier = jnp.dot(named.astype(F32).astype(BF), before, preferred_element_type=F32)
    slots[...] = jnp.where(named, earlier, -1.0)

    pl.semaphore_wait(barrier, count)

    tok_copy = remote(tok_own, tok_oth, ts, tr, dev(z, y, x, 1 - c))
    tok_copy.start()

    def w_src(px, py, pc):
        col = (py * 8 + px * 2 + pc) * half
        return w_ref.at[:, :, pl.ds(pl.multiple_of(col, half), half)]

    own_w = pltpu.make_async_copy(w_src(x, yl, c), wrecv.at[0, yl, c], own_sem)
    own_w.start()
    other_w = remote(w_src(x, yl, 1 - c), wrecv.at[0, yl, c], ws.at[0], wr.at[0, yl, c], dev(z, y, x, 1 - c))
    other_w.start()

    def w_relay(d, dy):
        pyl = yl if dy == 0 else 1 - yl
        step = 1 if d == 0 else -1
        return remote(
            w_src((x + 2) % 4, pyl, d), wrelay.at[d, dy], rs.at[d, dy], rr.at[d, dy],
            dev(z, y, x + step, c),
        )

    def w_direct(d, dy, pc):
        pyl = yl if dy == 0 else 1 - yl
        step = 1 if d == 0 else -1
        xrel = 3 if d == 0 else 1
        return remote(
            w_src((x + step) % 4, pyl, pc), wrecv.at[xrel, yl, c],
            ws.at[1 + (d * 2 + dy) * 2 + pc], wr.at[xrel, yl, c],
            dev(z, y if dy == 0 else yp, x + step, pc),
        )

    def w_cross(pc):
        return remote(
            w_src(x, 1 - yl, pc), wrecv.at[0, yl, c], ws.at[9 + pc], wr.at[0, yl, c],
            dev(z, yp, x, pc),
        )

    def w_forward(d, dy):
        step = 1 if d == 0 else -1
        return remote(
            wrelay.at[d, dy], wrecv.at[2, yl, c], fs.at[d, dy], wr.at[2, yl, c],
            dev(z, y if dy == 0 else yp, x + step, d),
        )

    for d in range(2):
        w_relay(d, 0).start()
    for pc in range(2):
        w_cross(pc).start()
    for d in range(2):
        for pc in range(2):
            w_direct(d, 0, pc).start()
    for d in range(2):
        w_relay(d, 1).start()
    for d in range(2):
        for pc in range(2):
            w_direct(d, 1, pc).start()

    got(tok_oth, tr)
    spread_r, spread_c = it(jnp.int32, (192, 384), 0), it(jnp.int32, (192, 384), 1)
    to_own = (spread_c == spread_r + c * 192).astype(F32).astype(BF)
    to_oth = (spread_c == spread_r + (1 - c) * 192).astype(F32).astype(BF)
    both = jnp.dot(tok_own[...], to_own, preferred_element_type=F32)
    both = both + jnp.dot(tok_oth[...], to_oth, preferred_element_type=F32)
    both = both.astype(BF)

    def place_of(o, js):
        oh, ol = (o % 8) // 2, o % 2
        return xbuf.at[
            js, c, 0, oh // 2,
            pl.ds(pl.multiple_of((oh % 2) * 48, 48), 48),
            pl.ds(pl.multiple_of(ol * 384, 384), 384),
        ]

    spot = it(jnp.int32, (CAP, 128), 0).astype(F32)
    for j in range(4):
        k = 2 * (3 - j) + c
        to = (z + 8 - k) % 8
        table = (slots[pl.ds(to, 1), :] == spot).astype(F32).astype(BF)
        placed[j] = jnp.dot(table, both, preferred_element_type=F32).astype(BF)
        if j < 3:
            remote(placed.at[j], place_of(y, j), zs.at[j], zr.at[j], dev(to, y, x, c)).start()
        else:
            @pl.when(c == 1)
            def _():
                remote(placed.at[j], place_of(y, j), zs.at[j], zr.at[j], dev(to, y, x, c)).start()

            @pl.when(c == 0)
            def _():
                pltpu.make_async_copy(placed.at[j], place_of(y, j), zl).start()

    def w_relayed(d, dy):
        got(wrelay.at[d, dy], rr.at[d, dy])
        w_forward(d, dy).start()

    def y_send(d, h, hf):
        o = y + 8 - (h - 1) if d == 0 else y + (h - 1)
        to = y + 1 if d == 0 else y + 7
        region = place_of(o, pl.ds(2 * hf, 2))
        return remote(region, region, ys.at[d, h - 1, hf], yr.at[d, h - 1, hf], dev(z, to, x, c))

    def y_got(d, h, hf):
        o = y + 8 - h if d == 0 else y + h
        got(place_of(o, pl.ds(2 * hf, 2)), yr.at[d, h - 1, hf])

    w_relayed(0, 0)
    w_relayed(1, 0)

    for hf in range(2):
        for j in (2 * hf, 2 * hf + 1):
            if j < 3:
                got(place_of(y, j), zr.at[j])
            else:
                @pl.when(c == 1)
                def _():
                    got(place_of(y, j), zr.at[j])

                @pl.when(c == 0)
                def _():
                    pltpu.make_async_copy(placed.at[j], place_of(y, j), zl).wait()
        y_send(0, 1, hf).start()
        y_send(1, 1, hf).start()
    for h in range(1, 4):
        for hf in range(2):
            for d in range(2):
                y_got(d, h, hf)
                if h < 3 or d == hf:
                    y_send(d, h + 1, hf).start()
        if h == 2:
            w_relayed(0, 1)
            w_relayed(1, 1)

    def unit(u):
        return u // 2, (u % 2 + yh // 2) % 2

    def x_own(u, d):
        j, hf = unit(u)
        return remote(
            xbuf.at[j, c, 0, hf], xbuf.at[j, c, 3 if d == 0 else 1, hf],
            xs.at[u, d], xr.at[u, d], dev(z, y, x + 1 if d == 0 else x + 3, c),
        )

    def x_half(u, d, xrel):
        j, hf = unit(u)
        return xbuf.at[j, c, xrel, hf, pl.ds(48 * d, 48)]

    def x_forward(u, d):
        return remote(
            x_half(u, d, 3 if d == 0 else 1), x_half(u, d, 2),
            xs.at[u, 2 + d], xr.at[u, 2 + d], dev(z, y, x + 1 if d == 0 else x + 3, c),
        )

    y_got(0, 4, 0)
    for u in range(2):
        x_own(u, 0).start()
        x_own(u, 1).start()
    y_got(1, 4, 1)

    two = 2 * rows
    pr, pc_ = it(jnp.int32, (two, two), 0), it(jnp.int32, (two, two), 1)
    apart = (pc_ == jnp.where(pr < rows, 2 * pr, 2 * (pr - rows) + 1)).astype(F32).astype(BF)

    def sort_piece(xrel, sl, sc):
        piece = wrecv[xrel, sl, sc].reshape(two, half)
        split = jnp.dot(apart, piece, preferred_element_type=F32).astype(BF)
        at = pl.ds(pl.multiple_of((sl * 2 + sc) * rows, rows), rows)
        wk[xrel, at, pl.ds(0, half)] = split[:rows]
        wk[xrel, at, pl.ds(half, half)] = split[rows:]

    own_w.wait()

    def take(i, carry):
        xrel, sl, sc = i // 4, (i // 2) % 2, i % 2
        mine = (xrel == 0) & (sl == yl) & (sc == c)

        @pl.when(jnp.logical_not(mine))
        def _():
            got(wrecv.at[xrel, sl, sc], wr.at[xrel, sl, sc])

        sort_piece(xrel, sl, sc)
        return carry

    lax.fori_loop(0, 16, take, 0)

    def swap(u):
        j, hf = unit(u)
        region = xbuf.at[j, c, :, hf]
        return remote(region, region, ds.at[u], dr.at[u], dev(z, y, x, 1 - c))

    def give(u, c2, q):
        j, hf = unit(u)
        k = 2 * (3 - j) + c2
        yhs = 2 * hf + q
        src = act.at[u, c2, pl.ds(48 * q, 48)]
        dst = ret.at[z, :, pl.ds(pl.multiple_of(yh * half, half), half)]
        mine = (k == 0) & (yhs == yh)
        return mine, src, dst, k, yhs

    def compute(u):
        j, hf = unit(u)
        acc = None
        for xrel in range(4):
            left = xbuf[j, :, xrel, hf].reshape(192, 768)
            part = jnp.dot(left, wk[xrel], preferred_element_type=F32)
            acc = part if acc is None else acc + part
        g, up = acc[:, :half], acc[:, half:]
        act[u] = (g / (1.0 + jnp.exp(-g)) * up).astype(BF).reshape(2, 96, half)
        for c2 in range(2):
            for q in range(2):
                mine, src, dst, k, yhs = give(u, c2, q)

                @pl.when(mine)
                def _():
                    pltpu.make_async_copy(src, dst, hl).start()

                @pl.when(jnp.logical_not(mine))
                def _():
                    remote(
                        src, dst, hs.at[k, yhs], hr.at[k, yh],
                        ((z + k) % 8 * 4 + yhs, b),
                    ).start()

    def turn(u, carry):
        @pl.when(u < 8)
        def _():
            for d in range(2):
                j, hf = unit(u)
                got(xbuf.at[j, c, 3 if d == 0 else 1, hf], xr.at[u, d])
                x_forward(u, d).start()

        @pl.when(u < 6)
        def _():
            for d in range(2):
                x_own(u + 2, d).start()

        @pl.when((u >= 1) & (u < 9))
        def _():
            for d in range(2):
                got(x_half(u - 1, d, 2), xr.at[u - 1, 2 + d])
            swap(u - 1).start()

        @pl.when(u >= 2)
        def _():
            j, hf = unit(u - 2)
            got(xbuf.at[j, 1 - c, :, hf], dr.at[u - 2])
            compute(u - 2)

        return carry

    lax.fori_loop(0, 10, turn, 0)

    ids = ids_ref[...]
    lane = it(jnp.int32, (128, 128), 1)
    row = it(jnp.int32, (128, 128), 0)
    names = ((ids[:, 0:1] == lane) | (ids[:, 1:2] == lane)).astype(F32)
    lower = (lane < row).astype(F32).astype(BF)
    ahead = jnp.dot(lower, names.astype(BF), preferred_element_type=F32)
    wide = it(jnp.int32, (128, E * CAP), 1).astype(F32)
    picks = []
    for kk in range(2):
        one = ids[:, kk : kk + 1]
        pos = jnp.sum(jnp.where(one == lane, ahead, 0.0), axis=1, keepdims=True)
        picks.append((wide == pos + one.astype(F32) * CAP).astype(F32).astype(BF))

    def back(i, carry):
        k, ys_ = i // 4, i % 4
        mine = (k == 0) & (ys_ == yh)
        src_z = (z + 8 - k) % 8
        dst = ret.at[src_z, :, pl.ds(pl.multiple_of(ys_ * half, half), half)]

        @pl.when(mine)
        def _():
            pltpu.make_async_copy(dst, dst, hl).wait()

        @pl.when(jnp.logical_not(mine))
        def _():
            got(dst, hr.at[k, ys_])
            sent(dst, hs.at[k, ys_])

        return carry

    lax.fori_loop(0, 32, back, 0)
    came = ret[...].reshape(E * CAP, 4 * half)
    for kk in range(2):
        out_ref[kk] = jnp.dot(picks[kk], came, preferred_element_type=F32).astype(BF)

    sent(tok_own, ts)
    piece = wrecv.at[0, 0, 0]
    for i in range(11):
        sent(piece, ws.at[i])
    for d in range(2):
        for dy in range(2):
            sent(piece, rs.at[d, dy])
            sent(piece, fs.at[d, dy])
    for j in range(3):
        sent(placed.at[j], zs.at[j])

    @pl.when(c == 1)
    def _():
        sent(placed.at[3], zs.at[3])

    for h in range(1, 5):
        for hf in range(2):
            for d in range(2):
                if h < 4 or d == hf:
                    sent(place_of(y, pl.ds(2 * hf, 2)), ys.at[d, h - 1, hf])

    def gone(u, carry):
        for d in range(2):
            sent(xbuf.at[0, c, 0, 0], xs.at[u, d])
            sent(x_half(0, d, 2), xs.at[u, 2 + d])
        sent(xbuf.at[0, c, :, 0], ds.at[u])
        return carry

    lax.fori_loop(0, 8, gone, 0)


def local(tokens, expert_ids, joined_weight):
    w = joined_weight[0]
    rows = w.shape[0]
    dma = pltpu.SemaphoreType.DMA
    vmem = pl.BlockSpec(memory_space=pltpu.VMEM)
    out = pl.pallas_call(
        kernel,
        out_shape=jax.ShapeDtypeStruct((2, 128, 1024), BF),
        in_specs=[vmem, vmem, vmem, pl.BlockSpec(memory_space=pltpu.HBM)],
        out_specs=vmem,
        scratch_shapes=[
            pltpu.VMEM((4, 2, 4, 2, 96, 768), BF),
            pltpu.VMEM((4, 2, 2, rows, 2, 256), BF),
            pltpu.VMEM((2, 2, rows, 2, 256), BF),
            pltpu.VMEM((4, 768, 512), BF),
            pltpu.VMEM((128, 192), BF),
            pltpu.VMEM((128, 192), BF),
            pltpu.VMEM((4, CAP, 384), BF),
            pltpu.VMEM((8, 128), F32),
            pltpu.VMEM((8, 2, 96, 256), BF),
            pltpu.VMEM((8, CAP, 1024), BF),
            dma((11,)), dma((4, 2, 2)), dma((2, 2)), dma((2, 2)), dma((2, 2)), dma,
            dma, dma, dma((4,)), dma((4,)), dma,
            dma((2, 4, 2)), dma((2, 4, 2)), dma((8, 4)), dma((8, 4)),
            dma((8,)), dma((8,)), dma((8, 4)), dma((8, 4)), dma,
        ],
        compiler_params=pltpu.CompilerParams(
            collective_id=0, has_side_effects=True, vmem_limit_bytes=60 * 1024 * 1024
        ),
    )(tokens, expert_ids, expert_ids.T, w)
    return out.reshape(2, 128, 4, 256).transpose(1, 0, 2, 3)


def solution(mesh):
    placed = (P("expert", "tensor"), P("expert", None), P("expert", "tensor", None, None))
    return jax.shard_map(
        local,
        mesh=mesh,
        in_specs=placed,
        out_specs=P("expert", None, None, "tensor"),
        check_vma=False,
    )
```

```python
import functools

import jax
import jax.numpy as jnp
from jax import lax
from jax.experimental import pallas as pl
from jax.experimental.pallas import tpu as pltpu
from jax.sharding import PartitionSpec as P

MESH = pl.DeviceIdType.MESH
E = 8
CAP = 48
BF = jnp.bfloat16
F32 = jnp.float32


def kernel(
    tok_ref, ids_ref, w_ref, out_ref,
    xbuf, wrecv, crelay, wk, tok, placed, slots, act, back_y, ret,
    ws, wsend, wr, cr, own_sem, ts, tr, zs, zr, zl,
    ys, yr, xs, xr, ns, nr, ds, dr, hs, hy, hyr, hr, hl,
):
    a, b = lax.axis_index("expert"), lax.axis_index("tensor")
    z, yh = a // 4, a % 4
    yl, x, c = b // 8, (b // 2) % 4, b % 2
    y = 2 * yh + yl

    def dev(zz, yy, xx, cc):
        yy, xx, zz = yy % 8, xx % 4, zz % 8
        return (zz * 4 + yy // 2, (yy % 2) * 8 + xx * 2 + cc)

    yp = y + 1 - 2 * yl
    rows = w_ref.shape[0]
    half = 256

    def remote(src, dst, send, recv, to):
        return pltpu.make_async_remote_copy(
            src_ref=src, dst_ref=dst, send_sem=send, recv_sem=recv,
            device_id=to, device_id_type=MESH,
        )

    me = dev(z, y, x, 1 - c)

    def got(ref, sem):
        remote(ref, ref, sem, sem, me).wait_recv()

    def sent(ref, sem):
        remote(ref, ref, sem, sem, me).wait_send()

    barrier = pltpu.get_barrier_semaphore()
    count = 0

    def greet(to):
        pl.semaphore_signal(barrier, inc=1, device_id=to, device_id_type=MESH)

    for dx in range(4):
        for dy in range(2):
            for dc in range(2):
                if dx or dy or dc:
                    greet(dev(z, y if dy == 0 else yp, x + dx, c if dc == 0 else 1 - c))
                    count += 1
    for k in range(1, 8):
        greet(dev(z + k, y, x, c))
        count += 1
    greet(dev(z, y - 1 + 2 * yl, x, c))
    count += 1

    tok[c] = tok_ref[...]
    it = lax.broadcasted_iota
    ids_t = ids_ref[...]
    named = (ids_t[0:1, :] == it(jnp.int32, (8, 128), 0)) | (ids_t[1:2, :] == it(jnp.int32, (8, 128), 0))
    before = (it(jnp.int32, (128, 128), 0) < it(jnp.int32, (128, 128), 1)).astype(F32).astype(BF)
    earlier = jnp.dot(named.astype(F32).astype(BF), before, preferred_element_type=F32)
    slots[...] = jnp.where(named, earlier, -1.0)

    pl.semaphore_wait(barrier, count)

    tok_copy = remote(tok.at[c], tok.at[c], ts, tr, dev(z, y, x, 1 - c))
    tok_copy.start()

    def w_src(px, py, pc):
        col = (py * 8 + px * 2 + pc) * half
        return w_ref.at[:, :, pl.ds(pl.multiple_of(col, half), half)]

    own_w = pltpu.make_async_copy(w_src(x, yl, c), wrecv.at[0, yl, c], own_sem)
    own_w.start()
    other_w = remote(w_src(x, yl, 1 - c), wrecv.at[0, yl, c], ws, wr.at[0, yl, c], dev(z, y, x, 1 - c))
    other_w.start()

    def along(d):
        return dev(z, y, x + 1 if d == 0 else x + 3, c)

    def w_direct(step, pc):
        return remote(
            w_src((x + step) % 4, yl, pc), wrecv.at[4 - step, yl, c],
            wsend, wr.at[4 - step, yl, c], dev(z, y, x + step, pc),
        )

    def w_cross(step, pc):
        src = w_src((x + step) % 4, 1 - yl, pc)
        if step == 0:
            return remote(src, wrecv.at[0, yl, c], wsend, wr.at[0, yl, c], dev(z, yp, x, pc))
        return remote(src, crelay.at[step - 1, pc], wsend, cr.at[step - 1, pc], dev(z, yp, x, c))

    def c_direct(step, pc):
        return remote(
            crelay.at[step - 1, pc], wrecv.at[4 - step, 1 - yl, c],
            wsend, wr.at[4 - step, 1 - yl, c], dev(z, y, x + step, pc),
        )

    for pc in range(2):
        w_direct(2, pc).start()
    for pc in range(2):
        w_cross(2, pc).start()
    for pc in range(2):
        for step in (1, 3):
            w_direct(step, pc).start()

    got(tok.at[1 - c], tr)
    both = tok[...].reshape(384, 128)

    def piece_of(o, xrel, start, size, cc):
        oh, ol = (o % 8) // 2, o % 2
        return xbuf.at[
            cc, xrel, oh, pl.ds(start, size), pl.ds(pl.multiple_of(ol * 384, 384), 384)
        ]

    spot = it(jnp.int32, (CAP, 128), 0).astype(F32)
    for j in range(4):
        k = (4, 6, 2, 0)[j] - c
        to = (z + 8 - k) % 8
        table = (slots[pl.ds(to, 1), :] == spot).astype(F32).astype(BF)
        placed[j] = lax.dot_general(
            table, both, (((1,), (1,)), ((), ())), preferred_element_type=F32
        ).astype(BF)
        if j < 3:
            remote(placed.at[j], piece_of(y, 0, 48 * j, 48, c), zs.at[j], zr.at[j], dev(to, y, x, c)).start()
        else:
            @pl.when(c == 1)
            def _():
                remote(placed.at[j], piece_of(y, 0, 48 * j, 48, c), zs.at[j], zr.at[j], dev(to, y, x, c)).start()

            @pl.when(c == 0)
            def _():
                pltpu.make_async_copy(placed.at[j], piece_of(y, 0, 48 * j, 48, c), zl).start()

    def y_send(d, h, hf):
        o = y + 8 - (h - 1) if d == 0 else y + (h - 1)
        to = y + 1 if d == 0 else y + 7
        region = piece_of(o, 0, 96 * hf, 96, c)
        return remote(region, region, ys.at[d, h - 1, hf], yr.at[d, h - 1, hf], dev(z, to, x, c))

    def y_got(d, h, hf):
        o = y + 8 - h if d == 0 else y + h
        got(piece_of(o, 0, 96 * hf, 96, c), yr.at[d, h - 1, hf])

    def y_round(h):
        for hf in range(2):
            for d in range(2):
                y_got(d, h, hf)
                if h < 3 or d == hf:
                    y_send(d, h + 1, hf).start()

    side = 2 * yl - 1

    def origin(v):
        away = (0, 0, -1, -1, -2, -3, 3, 4, 3, 4, -2, -3, 1, 1, 2, 2)[v]
        return (y + 8 + side * away) % 8

    def part(v, xrel, cc, start=0, size=96):
        o, near = origin(v), (0, 1, 0, 1, 0, 0, 0, 0, 1, 1, 1, 1, 0, 1, 0, 1)[v]
        return xbuf.at[
            cc, xrel, o // 2, pl.ds(96 * near + start, size),
            pl.ds(pl.multiple_of(o % 2 * 384, 384), 384),
        ]

    def x_own(v, d):
        return remote(
            part(v, 0, c), part(v, 3 if d == 0 else 1, c), xs, xr.at[v, d], along(d)
        )

    def x_forward(v, d):
        return remote(
            part(v, 3 if d == 0 else 1, c, 48 * d, 48), part(v, 2, c, 48 * d, 48),
            xs, xr.at[v, 2], along(d),
        )

    def x_start(u):
        for d in range(2):
            x_own(u, d).start()

    def c_directed(step, pc):
        got(crelay.at[step - 1, pc], cr.at[step - 1, pc])
        c_direct(step, pc).start()

    for hf in range(2):
        for j in (2 * hf, 2 * hf + 1):
            if j < 3:
                got(piece_of(y, 0, 48 * j, 48, c), zr.at[j])
            else:
                @pl.when(c == 1)
                def _():
                    got(piece_of(y, 0, 48 * j, 48, c), zr.at[j])

                @pl.when(c == 0)
                def _():
                    pltpu.make_async_copy(placed.at[j], piece_of(y, 0, 48 * j, 48, c), zl).wait()
        y_send(0, 1, hf).start()
        y_send(1, 1, hf).start()
    two = 2 * rows
    pr, pc_ = it(jnp.int32, (two, two), 0), it(jnp.int32, (two, two), 1)
    apart = (pc_ == jnp.where(pr < rows, 2 * pr, 2 * (pr - rows) + 1)).astype(F32).astype(BF)

    def sort_piece(xrel, sl, sc):
        piece = wrecv[xrel, sl, sc].reshape(two, half)
        split = jnp.dot(apart, piece, preferred_element_type=F32).astype(BF)
        at = pl.ds(pl.multiple_of((sl * 2 + sc) * rows, rows), rows)
        wk[xrel, at, pl.ds(0, half)] = split[:rows]
        wk[xrel, at, pl.ds(half, half)] = split[rows:]

    def take(row):
        def one(i, carry):
            xrel, sc = i // 2, i % 2
            mine = (xrel == 0) & (row == yl) & (sc == c)

            @pl.when(jnp.logical_not(mine))
            def _():
                got(wrecv.at[xrel, row, sc], wr.at[xrel, row, sc])

            sort_piece(xrel, row, sc)
            return carry

        lax.fori_loop(0, 8, one, 0)

    def swap(v):
        region = part(v, pl.ds(0, 4), c)
        return remote(region, region, ds, dr.at[v], dev(z, y, x, 1 - c))

    def gather(v):
        for d in range(2):
            got(part(v, 3 if d == 0 else 1, c), xr.at[v, d])
            x_forward(v, d).start()
        if v < 10:
            x_start(v + 2)

    def collect(v):
        got(part(v, 2, c), xr.at[v, 2])
        swap(v).start()
        if v < 4:
            region = part(v, pl.ds(1, 3), c)
            remote(region, region, ns, nr.at[v], dev(z, y + side + 8, x, c)).start()

    def collect_near(v):
        got(part(v, pl.ds(1, 3), c), nr.at[v - 12])
        swap(v).start()

    firsts, lasts = (0, 1, 12, 13, 4, 10, 6, 8), (2, 3, 14, 15, 5, 11, 7, 9)

    def hand(store, i, by, to):
        for c2 in range(2):
            for q in range(2):
                k = ((2 - 2 * q if i % 2 else 4 + 2 * q) - c2) % 8
                src = store.at[4 * i + 2 * c2 + q]
                dst = ret.at[z, :, pl.ds(pl.multiple_of(by * half, half), half)]
                if k == 0 and to is yh:
                    pltpu.make_async_copy(src, dst, hl.at[by]).start()
                else:
                    remote(src, dst, hs, hr.at[k, by], ((z + k) % 8 * 4 + to, b)).start()

    def giver(i):
        return (yh + 8 - (origin(lasts[i]) // 2 - yh)) % 4

    def pass_on(i):
        got(back_y.at[pl.ds(4 * i, 4)], hyr.at[i])
        hand(back_y, i, giver(i), yh)

    def finish(i):
        first, last, near = firsts[i], lasts[i], i % 2
        got(part(first, pl.ds(0, 4), 1 - c), dr.at[first])
        got(part(last, pl.ds(0, 4), 1 - c), dr.at[last])
        yhs = origin(last) // 2
        acc = None
        for xrel in range(4):
            left = xbuf[:, xrel, yhs, pl.ds(96 * near, 96), :].reshape(192, 768)
            term = jnp.dot(left, wk[xrel], preferred_element_type=F32)
            acc = term if acc is None else acc + term
        g, up = acc[:, :half], acc[:, half:]
        act[pl.ds(4 * i, 4)] = (g / (1.0 + jnp.exp(-g)) * up).astype(BF).reshape(4, CAP, half)
        if i < 2:
            hand(act, i, yh, yh)
        elif i == 5:
            hand(act, i, yh, yhs)
        else:
            mine = act.at[pl.ds(4 * i, 4)]
            remote(mine, back_y.at[pl.ds(4 * i, 4)], hy, hyr.at[i], (z * 4 + yhs, b)).start()

    x_start(0)
    x_start(1)
    w_cross(1, 0).start()
    for pc in range(2):
        c_directed(2, pc)
    y_round(1)
    w_cross(3, 0).start()
    y_round(2)
    w_cross(1, 1).start()
    c_directed(1, 0)
    gather(0)
    gather(1)
    y_round(3)
    w_cross(3, 1).start()
    for pc in range(2):
        w_cross(0, pc).start()
    c_directed(3, 0)
    c_directed(1, 1)
    gather(2)
    collect(0)
    collect(1)
    own_w.wait()
    take(yl)
    c_directed(3, 1)
    gather(3)
    gather(4)
    y_got(0, 4, 0)
    y_got(1, 4, 1)
    collect(2)
    collect(3)
    gather(5)
    take(1 - yl)
    collect_near(12)
    collect_near(13)
    finish(0)
    gather(6)
    finish(1)
    collect(4)
    collect(5)
    gather(7)
    finish(4)
    gather(8)
    collect(6)
    collect_near(14)
    collect(7)
    finish(6)
    gather(9)
    collect_near(15)
    finish(2)
    pass_on(4)
    gather(10)
    collect(8)
    finish(3)
    collect(9)
    gather(11)
    pass_on(2)
    finish(7)
    collect(10)
    pass_on(6)
    pass_on(3)
    collect(11)
    finish(5)
    pass_on(7)

    chosen = None
    for kk in range(2):
        one = ids_t[kk : kk + 1, :]
        pos = jnp.sum(jnp.where(one == it(jnp.int32, (8, 128), 0), earlier, 0.0), axis=0, keepdims=True)
        spread = (it(jnp.int32, (128, 256), 1) == 2 * it(jnp.int32, (128, 256), 0) + kk).astype(F32).astype(BF)
        pair = jnp.concatenate([one.astype(F32), pos, jnp.zeros((6, 128), F32)], axis=0).astype(BF)
        part = jnp.dot(pair, spread, preferred_element_type=F32)
        chosen = part if chosen is None else chosen + part
    took = chosen[0:1, :] * CAP + chosen[1:2, :]
    pick = (it(jnp.int32, (E * CAP, 256), 0).astype(F32) == took).astype(F32).astype(BF)

    def back(i, carry):
        k, by = i // 4, i % 4
        dst = ret.at[(z + 8 - k) % 8, :, pl.ds(pl.multiple_of(by * half, half), half)]

        stays = (k == 0) & (by != giver(5))

        @pl.when(stays)
        def _():
            pltpu.make_async_copy(dst, dst, hl.at[by]).wait()

        @pl.when(jnp.logical_not(stays))
        def _():
            got(dst, hr.at[k, by])

        return carry

    lax.fori_loop(0, 32, back, 0)
    came = ret[...].reshape(E * CAP, 4 * half)
    out_ref[...] = lax.dot_general(
        pick, came, (((0,), (0,)), ((), ())), preferred_element_type=F32
    ).astype(BF)

    sent(tok.at[c], ts)
    sent(wrecv.at[0, 0, 0], ws)
    sent(xbuf.at[c, :, :, pl.ds(0, 160)], wsend)
    sent(xbuf.at[c, pl.ds(0, 3), pl.ds(0, 3)], xs)
    sent(xbuf.at[c, 0, pl.ds(0, 3)], ns)
    sent(xbuf.at[c], ds)
    sent(act.at[pl.ds(0, 29)], hs)
    sent(act.at[pl.ds(0, 20)], hy)
    for j in range(3):
        sent(placed.at[j], zs.at[j])

    @pl.when(c == 1)
    def _():
        sent(placed.at[3], zs.at[3])

    for h in range(1, 5):
        for hf in range(2):
            for d in range(2):
                if h < 4 or d == hf:
                    sent(piece_of(y, 0, 96 * hf, 96, c), ys.at[d, h - 1, hf])


def local(tokens, expert_ids, joined_weight):
    w = joined_weight[0]
    rows = w.shape[0]
    dma = pltpu.SemaphoreType.DMA
    vmem = pl.BlockSpec(memory_space=pltpu.VMEM)
    out = pl.pallas_call(
        kernel,
        out_shape=jax.ShapeDtypeStruct((256, 1024), BF),
        in_specs=[vmem, vmem, pl.BlockSpec(memory_space=pltpu.HBM)],
        out_specs=vmem,
        scratch_shapes=[
            pltpu.VMEM((2, 4, 4, 192, 768), BF),
            pltpu.VMEM((4, 2, 2, rows, 2, 256), BF),
            pltpu.VMEM((3, 2, rows, 2, 256), BF),
            pltpu.VMEM((4, 768, 512), BF),
            pltpu.VMEM((2, 192, 128), BF),
            pltpu.VMEM((4, CAP, 384), BF),
            pltpu.VMEM((8, 128), F32),
            pltpu.VMEM((32, CAP, 256), BF),
            pltpu.VMEM((32, CAP, 256), BF),
            pltpu.VMEM((8, CAP, 1024), BF),
            dma, dma, dma((4, 2, 2)), dma((3, 2)), dma,
            dma, dma, dma((4,)), dma((4,)), dma,
            dma((2, 4, 2)), dma((2, 4, 2)), dma, dma((12, 3)), dma, dma((4,)),
            dma, dma((16,)), dma, dma, dma((8,)), dma((8, 4)), dma((4,)),
        ],
        compiler_params=pltpu.CompilerParams(
            collective_id=0, has_side_effects=True, vmem_limit_bytes=60 * 1024 * 1024
        ),
    )(tokens.T, expert_ids.T, w)
    return out.reshape(128, 2, 4, 256)


def solution(mesh):
    placed = (P("expert", "tensor"), P("expert", None), P("expert", "tensor", None, None))
    return jax.shard_map(
        local,
        mesh=mesh,
        in_specs=placed,
        out_specs=P("expert", None, None, "tensor"),
        check_vma=False,
    )
```

```python
import functools

import jax
import jax.numpy as jnp
from jax import lax
from jax.experimental import pallas as pl
from jax.experimental.pallas import tpu as pltpu
from jax.sharding import PartitionSpec as P

MESH = pl.DeviceIdType.MESH
E = 8
CAP = 48
BF = jnp.bfloat16
F32 = jnp.float32


def kernel(
    tok_ref, ids_ref, w_ref, out_ref,
    xbuf, wrecv, crelay, wk, tok, placed, slots, act, back_y, ret, rows_out, packed,
    ws, wsend, wr, cr, own_sem, ts, tr, zs, zr, zl,
    ys, yr, xs, xr, ns, nr, ds, dr, hs, hy, hyr, hr, hl,
):
    a, b = lax.axis_index("expert"), lax.axis_index("tensor")
    z, yh = a // 4, a % 4
    yl, x, c = b // 8, (b // 2) % 4, b % 2
    y = 2 * yh + yl

    def dev(zz, yy, xx, cc):
        yy, xx, zz = yy % 8, xx % 4, zz % 8
        return (zz * 4 + yy // 2, (yy % 2) * 8 + xx * 2 + cc)

    yp = y + 1 - 2 * yl
    rows = w_ref.shape[0]
    half = 256

    def remote(src, dst, send, recv, to):
        return pltpu.make_async_remote_copy(
            src_ref=src, dst_ref=dst, send_sem=send, recv_sem=recv,
            device_id=to, device_id_type=MESH,
        )

    me = dev(z, y, x, 1 - c)

    def got(ref, sem):
        remote(ref, ref, sem, sem, me).wait_recv()

    def sent(ref, sem):
        remote(ref, ref, sem, sem, me).wait_send()

    barrier = pltpu.get_barrier_semaphore()
    count = 0

    def greet(to):
        pl.semaphore_signal(barrier, inc=1, device_id=to, device_id_type=MESH)

    for dx in range(4):
        for dy in range(2):
            for dc in range(2):
                if dx or dy or dc:
                    greet(dev(z, y if dy == 0 else yp, x + dx, c if dc == 0 else 1 - c))
                    count += 1
    for k in range(1, 8):
        greet(dev(z + k, y, x, c))
        count += 1
    greet(dev(z, y - 1 + 2 * yl, x, c))
    count += 1

    tok[c] = tok_ref[...]
    it = lax.broadcasted_iota
    ids_t = ids_ref[...]
    named = (ids_t[0:1, :] == it(jnp.int32, (8, 128), 0)) | (ids_t[1:2, :] == it(jnp.int32, (8, 128), 0))
    before = (it(jnp.int32, (128, 128), 0) < it(jnp.int32, (128, 128), 1)).astype(F32).astype(BF)
    earlier = jnp.dot(named.astype(F32).astype(BF), before, preferred_element_type=F32)
    slots[...] = jnp.where(named, earlier, -1.0)

    pl.semaphore_wait(barrier, count)

    tok_copy = remote(tok.at[c], tok.at[c], ts, tr, dev(z, y, x, 1 - c))
    tok_copy.start()

    def w_src(px, py, pc):
        col = (py * 8 + px * 2 + pc) * half
        return w_ref.at[:, :, pl.ds(pl.multiple_of(col, half), half)]

    own_w = pltpu.make_async_copy(w_src(x, yl, c), wrecv.at[0, yl, c], own_sem)
    own_w.start()
    other_w = remote(w_src(x, yl, 1 - c), wrecv.at[0, yl, c], ws, wr.at[0, yl, c], dev(z, y, x, 1 - c))
    other_w.start()

    def along(d):
        return dev(z, y, x + 1 if d == 0 else x + 3, c)

    def w_direct(step, pc):
        return remote(
            w_src((x + step) % 4, yl, pc), wrecv.at[4 - step, yl, c],
            wsend, wr.at[4 - step, yl, c], dev(z, y, x + step, pc),
        )

    def w_cross(step, pc):
        src = w_src((x + step) % 4, 1 - yl, pc)
        if step == 0:
            return remote(src, wrecv.at[0, yl, c], wsend, wr.at[0, yl, c], dev(z, yp, x, pc))
        return remote(src, crelay.at[step - 1, pc], wsend, cr.at[step - 1, pc], dev(z, yp, x, c))

    def c_direct(step, pc):
        return remote(
            crelay.at[step - 1, pc], wrecv.at[4 - step, 1 - yl, c],
            wsend, wr.at[4 - step, 1 - yl, c], dev(z, y, x + step, pc),
        )

    for pc in range(2):
        w_direct(2, pc).start()
    for pc in range(2):
        w_cross(2, pc).start()
    for step in (1, 3):
        w_direct(step, 0).start()

    got(tok.at[1 - c], tr)
    both = tok[...].reshape(384, 128)

    def piece_of(o, xrel, start, size, cc):
        oh, ol = (o % 8) // 2, o % 2
        return xbuf.at[
            cc, xrel, oh, pl.ds(start, size), pl.ds(pl.multiple_of(ol * 384, 384), 384)
        ]

    spot = it(jnp.int32, (CAP, 128), 0).astype(F32)
    for j in range(4):
        k = (4, 6, 2, 0)[j] - c
        to = (z + 8 - k) % 8
        table = (slots[pl.ds(to, 1), :] == spot).astype(F32).astype(BF)
        placed[j] = lax.dot_general(
            table, both, (((1,), (1,)), ((), ())), preferred_element_type=F32
        ).astype(BF)
        if j < 3:
            remote(placed.at[j], piece_of(y, 0, 48 * j, 48, c), zs.at[j], zr.at[j], dev(to, y, x, c)).start()
        else:
            @pl.when(c == 1)
            def _():
                remote(placed.at[j], piece_of(y, 0, 48 * j, 48, c), zs.at[j], zr.at[j], dev(to, y, x, c)).start()

            @pl.when(c == 0)
            def _():
                pltpu.make_async_copy(placed.at[j], piece_of(y, 0, 48 * j, 48, c), zl).start()

    def y_send(d, h, hf):
        o = y + 8 - (h - 1) if d == 0 else y + (h - 1)
        to = y + 1 if d == 0 else y + 7
        region = piece_of(o, 0, 96 * hf, 96, c)
        return remote(region, region, ys.at[d, h - 1, hf], yr.at[d, h - 1, hf], dev(z, to, x, c))

    def y_got(d, h, hf):
        o = y + 8 - h if d == 0 else y + h
        got(piece_of(o, 0, 96 * hf, 96, c), yr.at[d, h - 1, hf])

    def y_round(h):
        for hf in range(2):
            for d in range(2):
                y_got(d, h, hf)
                if h < 3 or d == hf:
                    y_send(d, h + 1, hf).start()

    side = 2 * yl - 1

    def origin(v):
        away = (0, 0, -1, -1, -2, -3, 3, 4, 3, 4, -2, -3, 1, 1, 2, 2)[v]
        return (y + 8 + side * away) % 8

    def part(v, xrel, cc, start=0, size=96):
        o, near = origin(v), (0, 1, 0, 1, 0, 0, 0, 0, 1, 1, 1, 1, 0, 1, 0, 1)[v]
        return xbuf.at[
            cc, xrel, o // 2, pl.ds(96 * near + start, size),
            pl.ds(pl.multiple_of(o % 2 * 384, 384), 384),
        ]

    def x_own(v, d):
        return remote(
            part(v, 0, c), part(v, 3 if d == 0 else 1, c), xs, xr.at[v, d], along(d)
        )

    def x_forward(v, d):
        return remote(
            part(v, 3 if d == 0 else 1, c, 48 * d, 48), part(v, 2, c, 48 * d, 48),
            xs, xr.at[v, 2], along(d),
        )

    def x_start(u):
        for d in range(2):
            x_own(u, d).start()

    def c_directed(step, pc):
        got(crelay.at[step - 1, pc], cr.at[step - 1, pc])
        c_direct(step, pc).start()

    for hf in range(2):
        for j in (2 * hf, 2 * hf + 1):
            if j < 3:
                got(piece_of(y, 0, 48 * j, 48, c), zr.at[j])
            else:
                @pl.when(c == 1)
                def _():
                    got(piece_of(y, 0, 48 * j, 48, c), zr.at[j])

                @pl.when(c == 0)
                def _():
                    pltpu.make_async_copy(placed.at[j], piece_of(y, 0, 48 * j, 48, c), zl).wait()
        y_send(0, 1, hf).start()
        y_send(1, 1, hf).start()
    two = 2 * rows
    pr, pc_ = it(jnp.int32, (two, two), 0), it(jnp.int32, (two, two), 1)
    apart = (pc_ == jnp.where(pr < rows, 2 * pr, 2 * (pr - rows) + 1)).astype(F32).astype(BF)

    def sort_piece(xrel, sl, sc):
        piece = wrecv[xrel, sl, sc].reshape(two, half)
        split = jnp.dot(apart, piece, preferred_element_type=F32).astype(BF)
        at = pl.ds(pl.multiple_of((sl * 2 + sc) * rows, rows), rows)
        wk[xrel, at, pl.ds(0, half)] = split[:rows]
        wk[xrel, at, pl.ds(half, half)] = split[rows:]

    def take(row):
        def one(i, carry):
            xrel, sc = i // 2, i % 2
            mine = (xrel == 0) & (row == yl) & (sc == c)

            @pl.when(jnp.logical_not(mine))
            def _():
                got(wrecv.at[xrel, row, sc], wr.at[xrel, row, sc])

            sort_piece(xrel, row, sc)
            return carry

        lax.fori_loop(0, 8, one, 0)

    def swap(v):
        region = part(v, pl.ds(0, 4), c)
        return remote(region, region, ds, dr.at[v], dev(z, y, x, 1 - c))

    def gather(v):
        for d in range(2):
            got(part(v, 3 if d == 0 else 1, c), xr.at[v, d])
            x_forward(v, d).start()
        for later in ((), (), (), (), (6,), (7, 8), (9,), (10,), (11,), (), (), ())[v]:
            x_start(later)

    def collect(v):
        got(part(v, 2, c), xr.at[v, 2])
        swap(v).start()
        if v < 4:
            region = part(v, pl.ds(1, 3), c)
            remote(region, region, ns, nr.at[v], dev(z, y + side + 8, x, c)).start()

    def collect_near(v):
        got(part(v, pl.ds(1, 3), c), nr.at[v - 12])
        swap(v).start()

    firsts, lasts = (0, 1, 12, 13, 4, 10, 6, 8), (2, 3, 14, 15, 5, 11, 7, 9)

    def hand(store, i, by, to):
        for c2 in range(2):
            for q in range(2):
                k = ((2 - 2 * q if i % 2 else 4 + 2 * q) - c2) % 8
                src = store.at[4 * i + 2 * c2 + q]
                dst = ret.at[z, :, pl.ds(pl.multiple_of(by * half, half), half)]
                if k == 0 and to is yh:
                    pltpu.make_async_copy(src, dst, hl.at[by]).start()
                else:
                    remote(src, dst, hs, hr.at[k, by], ((z + k) % 8 * 4 + to, b)).start()

    def giver(i):
        return (yh + 8 - (origin(lasts[i]) // 2 - yh)) % 4

    def pass_on(i):
        got(back_y.at[pl.ds(4 * i, 4)], hyr.at[i])
        hand(back_y, i, giver(i), yh)

    def finish(i):
        first, last, near = firsts[i], lasts[i], i % 2
        got(part(first, pl.ds(0, 4), 1 - c), dr.at[first])
        got(part(last, pl.ds(0, 4), 1 - c), dr.at[last])
        yhs = origin(last) // 2
        acc = None
        for xrel in range(4):
            left = xbuf[:, xrel, yhs, pl.ds(96 * near, 96), :].reshape(192, 768)
            term = jnp.dot(left, wk[xrel], preferred_element_type=F32)
            acc = term if acc is None else acc + term
        g, up = acc[:, :half], acc[:, half:]
        act[pl.ds(4 * i, 4)] = (g / (1.0 + jnp.exp(-g)) * up).astype(BF).reshape(4, CAP, half)
        if i < 2:
            hand(act, i, yh, yh)
        elif i in (5, 7):
            hand(act, i, yh, yhs)
        else:
            mine = act.at[pl.ds(4 * i, 4)]
            remote(mine, back_y.at[pl.ds(4 * i, 4)], hy, hyr.at[i], (z * 4 + yhs, b)).start()

    x_start(0)
    x_start(1)
    for step in (1, 3):
        w_direct(step, 1).start()
    w_cross(1, 0).start()
    y_round(1)
    w_cross(3, 0).start()
    x_start(2)
    x_start(3)
    gather(0)
    gather(1)
    c_directed(2, 0)
    y_round(2)
    w_cross(1, 1).start()
    gather(2)
    gather(3)
    c_directed(2, 1)
    c_directed(1, 0)
    c_directed(3, 0)
    collect(0)
    y_round(3)
    w_cross(3, 1).start()
    for pc in range(2):
        w_cross(0, pc).start()
    x_start(4)
    x_start(5)
    collect(1)
    collect(2)
    c_directed(1, 1)
    collect(3)
    own_w.wait()
    take(yl)
    c_directed(3, 1)
    y_got(0, 4, 0)
    y_got(1, 4, 1)
    collect_near(12)
    gather(4)
    gather(5)
    collect_near(13)
    take(1 - yl)
    gather(6)
    collect_near(14)
    collect(4)
    collect(5)
    finish(0)
    finish(2)
    gather(7)
    finish(4)
    collect_near(15)
    finish(1)
    collect(6)
    gather(8)
    finish(3)
    collect(7)
    gather(9)
    finish(6)
    collect(8)
    gather(10)
    pass_on(2)
    collect(9)
    gather(11)
    pass_on(4)
    finish(7)
    collect(10)
    collect(11)
    finish(5)
    pass_on(3)
    pass_on(6)

    chosen = None
    for kk in range(2):
        one = ids_t[kk : kk + 1, :]
        pos = jnp.sum(jnp.where(one == it(jnp.int32, (8, 128), 0), earlier, 0.0), axis=0, keepdims=True)
        spread = (it(jnp.int32, (128, 256), 1) == 2 * it(jnp.int32, (128, 256), 0) + kk).astype(F32).astype(BF)
        pair = jnp.concatenate([one.astype(F32), pos, jnp.zeros((6, 128), F32)], axis=0).astype(BF)
        part = jnp.dot(pair, spread, preferred_element_type=F32)
        chosen = part if chosen is None else chosen + part
    took = chosen[0:1, :] * CAP + chosen[1:2, :]
    pick = (it(jnp.int32, (E * CAP, 256), 0).astype(F32) == took).astype(F32).astype(BF)

    def back(i, carry):
        k, by = i // 4, i % 4
        dst = ret.at[(z + 8 - k) % 8, :, pl.ds(pl.multiple_of(by * half, half), half)]

        stays = (k == 0) & (by != giver(5)) & (by != giver(7))

        @pl.when(stays)
        def _():
            pltpu.make_async_copy(dst, dst, hl.at[by]).wait()

        @pl.when(jnp.logical_not(stays))
        def _():
            got(dst, hr.at[k, by])

        return carry

    lax.fori_loop(0, 32, back, 0)
    came = ret[...].reshape(E * CAP, 4 * half)
    total = lax.dot_general(
        pick, came, (((0,), (0,)), ((), ())), preferred_element_type=F32
    )
    for r in range(4):
        for h in range(2):
            at = (2 * r + h) * 128
            rows_out[pl.ds(4 * h + r, 256, stride=8), :] = total[:, at : at + 128]
    packed[...] = rows_out[...].astype(BF)
    leave = pltpu.make_async_copy(packed, out_ref, own_sem)
    leave.start()

    sent(tok.at[c], ts)
    sent(wrecv.at[0, 0, 0], ws)
    sent(xbuf.at[c, :, :, pl.ds(0, 160)], wsend)
    sent(xbuf.at[c, pl.ds(0, 3), pl.ds(0, 3)], xs)
    sent(xbuf.at[c, 0, pl.ds(0, 3)], ns)
    sent(xbuf.at[c], ds)
    sent(act.at[pl.ds(0, 30)], hs)
    sent(act.at[pl.ds(0, 16)], hy)
    for j in range(3):
        sent(placed.at[j], zs.at[j])

    @pl.when(c == 1)
    def _():
        sent(placed.at[3], zs.at[3])

    for h in range(1, 5):
        for hf in range(2):
            for d in range(2):
                if h < 4 or d == hf:
                    sent(piece_of(y, 0, 96 * hf, 96, c), ys.at[d, h - 1, hf])
    leave.wait()


def local(tokens, expert_ids, joined_weight):
    w = joined_weight[0]
    rows = w.shape[0]
    dma = pltpu.SemaphoreType.DMA
    vmem = pl.BlockSpec(memory_space=pltpu.VMEM)
    out = pl.pallas_call(
        kernel,
        out_shape=jax.ShapeDtypeStruct((2048, 128), BF),
        in_specs=[vmem, vmem, pl.BlockSpec(memory_space=pltpu.HBM)],
        out_specs=pl.BlockSpec(memory_space=pl.ANY),
        scratch_shapes=[
            pltpu.VMEM((2, 4, 4, 192, 768), BF),
            pltpu.VMEM((4, 2, 2, rows, 2, 256), BF),
            pltpu.VMEM((3, 2, rows, 2, 256), BF),
            pltpu.VMEM((4, 768, 512), BF),
            pltpu.VMEM((2, 192, 128), BF),
            pltpu.VMEM((4, CAP, 384), BF),
            pltpu.VMEM((8, 128), F32),
            pltpu.VMEM((32, CAP, 256), BF),
            pltpu.VMEM((32, CAP, 256), BF),
            pltpu.VMEM((8, CAP, 1024), BF),
            pltpu.VMEM((2048, 128), F32),
            pltpu.VMEM((2048, 128), BF),
            dma, dma, dma((4, 2, 2)), dma((3, 2)), dma,
            dma, dma, dma((4,)), dma((4,)), dma,
            dma((2, 4, 2)), dma((2, 4, 2)), dma, dma((12, 3)), dma, dma((4,)),
            dma, dma((16,)), dma, dma, dma((8,)), dma((8, 4)), dma((4,)),
        ],
        compiler_params=pltpu.CompilerParams(
            collective_id=0, has_side_effects=True, vmem_limit_bytes=54000000
        ),
    )(tokens.T, expert_ids.T, w)
    return out.reshape(128, 2, 2, 4, 128).transpose(0, 1, 3, 2, 4).reshape(128, 2, 4, 256)


def solution(mesh):
    placed = (P("expert", "tensor"), P("expert", None), P("expert", "tensor", None, None))
    return jax.shard_map(
        local,
        mesh=mesh,
        in_specs=placed,
        out_specs=P("expert", None, None, "tensor"),
        check_vma=False,
    )
```
